256 devices in a mesh: clip: 64 (over x, z, core), row: 4 (over y).
Axes of the slice: x: 4, y: 4, z: 8, core: 2. Of those that a mesh axis runs over, the one named last changes fastest.
Arguments:
- features: bfloat16 [64, 128, 32, 256], P('clip', None, 'row'), may hold values from -6 to 6
- out_weight: bfloat16 [3, 128, 3, 3], replicated, may hold values from -0.1875 to 0.1875
- out_bias: float32 [3], replicated, may hold values from -0.5 to 0.5
- targets: bfloat16 [64, 3, 32, 256], P('clip', None, 'row'), may hold values from -1 to 1
- weight_one: bfloat16 [64, 3, 3, 3], replicated, may hold values from -1.25 to 1.25
- bias_one: float32 [64], replicated, may hold values from -0.2 to 0.2
- weight_two: bfloat16 [64, 64, 3, 3], replicated, may hold values from -0.375 to 0.375
- bias_two: float32 [64], replicated, may hold values from -0.2 to 0.2
- weight_three: bfloat16 [128, 64, 3, 3], replicated, may hold values from -0.375 to 0.375
- bias_three: float32 [128], replicated, may hold values from -0.2 to 0.2
- weight_four: bfloat16 [128, 128, 3, 3], replicated, may hold values from -0.25 to 0.25
- bias_four: float32 [128], replicated, may hold values from -0.2 to 0.2
- lin_one: float32 [64], replicated, may hold values from 0.05 to 0.5
- lin_two: float32 [128], replicated, may hold values from 0.05 to 0.5
Outputs:
- loss: float32 [], replicated
- feature_grad: bfloat16 [64, 128, 32, 256], P('clip', None, 'row')
- out_weight_grad: float32 [3, 128, 3, 3], replicated
- out_bias_grad: float32 [3], replicated
The draws below stay inside these ranges and needn't reach their ends.
All inputs are finite; a program needn't handle non-finite values.
Results may differ from the reference program's by a relative error of at most 0.02.
Values may be sent and summed in bfloat16 or wider, within the bound.
A program may use at most 64 MiB of HBM per device.

```python
import math
import jax
import jax.numpy as jnp
from jax import lax

CF = 128
C1 = 64
C2 = 128
W = 256
H = 32
FRAMES = 64


def shard_levels(own_key, extent, split, least, top_value):
    def one(dim, blocks):
        steps = jax.random.uniform(jax.random.fold_in(jax.random.fold_in(own_key, 6), dim), (blocks,), jnp.float32, least / len(split), top_value / len(split))
        return jnp.repeat(jnp.exp(steps), extent[dim] // blocks).reshape((-1,) + (1,) * (len(extent) - dim - 1))

    gain = one(*split[0])
    for cut in split[1:]:
        gain = gain * one(*cut)
    return gain


def gaussian(rng, dims, scale, limit, shards=(), kind=jnp.bfloat16):
    entries = scale * jax.random.normal(rng, dims, jnp.float32)
    if shards:
        entries = entries * shard_levels(rng, dims, shards, -0.22, 0.18)
    return jnp.clip(entries, -limit, limit).astype(kind)


def setup_inputs(seed: int = 0) -> dict:
    streams_of = jax.random.split(jax.random.key(seed), 15)
    features = gaussian(streams_of[0], (FRAMES, CF, H, W), 1.0, 6.0, ((0, 64), (2, 4)))
    out_weight = gaussian(streams_of[1], (3, CF, 3, 3), (9 * CF) ** -0.5, 0.1875)
    out_bias = jnp.clip(jax.random.uniform(streams_of[2], (3,), jnp.float32, -0.5, 0.5), -0.5, 0.5)
    targets = jnp.clip(jax.random.uniform(streams_of[3], (FRAMES, 3, H, W), jnp.float32, -1.0, 1.0) * shard_levels(streams_of[3], (FRAMES, 3, H, W), ((0, 64), (2, 4)), -0.4, 0.0), -1.0, 1.0).astype(jnp.bfloat16)
    weight_one = gaussian(streams_of[4], (C1, 3, 3, 3), 27 ** -0.5, 1.25)
    bias_one = jnp.clip(jax.random.uniform(streams_of[5], (C1,), jnp.float32, -0.2, 0.2), -0.2, 0.2)
    weight_two = gaussian(streams_of[6], (C1, C1, 3, 3), (9 * C1 // 2) ** -0.5, 0.375)
    bias_two = jnp.clip(jax.random.uniform(streams_of[7], (C1,), jnp.float32, -0.2, 0.2), -0.2, 0.2)
    weight_three = gaussian(streams_of[8], (C2, C1, 3, 3), (9 * C1 // 2) ** -0.5, 0.375)
    bias_three = jnp.clip(jax.random.uniform(streams_of[9], (C2,), jnp.float32, -0.2, 0.2), -0.2, 0.2)
    weight_four = gaussian(streams_of[10], (C2, C2, 3, 3), (9 * C2 // 2) ** -0.5, 0.25)
    bias_four = jnp.clip(jax.random.uniform(streams_of[11], (C2,), jnp.float32, -0.2, 0.2), -0.2, 0.2)
    lin_one = jnp.clip(jnp.exp(jax.random.uniform(streams_of[12], (C1,), jnp.float32, math.log(0.05), math.log(0.5))), 0.05, 0.5)
    lin_two = jnp.clip(jnp.exp(jax.random.uniform(streams_of[13], (C2,), jnp.float32, math.log(0.05), math.log(0.5))), 0.05, 0.5)
    return {"features": features, "out_weight": out_weight, "out_bias": out_bias, "targets": targets, "weight_one": weight_one, "bias_one": bias_one, "weight_two": weight_two, "bias_two": bias_two, "weight_three": weight_three, "bias_three": bias_three, "weight_four": weight_four, "bias_four": bias_four, "lin_one": lin_one, "lin_two": lin_two}


shift_values = [-0.03, -0.088, -0.188]
scale_values = [0.458, 0.448, 0.45]

def shift_array():
    return jnp.array(shift_values, jnp.float32).reshape(1, 3, 1, 1)

def scale_array():
    return jnp.array(scale_values, jnp.float32).reshape(1, 3, 1, 1)

def gelu_exact(values):
    return values * 0.5 * (1.0 + jax.scipy.special.erf(values / math.sqrt(2.0)))

def gelu_slope(values):
    normal_cdf = 0.5 * (1.0 + jax.scipy.special.erf(values / math.sqrt(2.0)))
    density = jnp.exp(-0.5 * values * values) / math.sqrt(2.0 * math.pi)
    return normal_cdf + values * density

def pad_rows(inputs):
    return jnp.pad(inputs, ((0, 0), (0, 0), (1, 1), (0, 0)))

def flipped(weight):
    return jnp.flip(weight, (2, 3)).transpose(1, 0, 2, 3)

def conv_valid(padded, weight):
    frame_count, channels, row_total, col_count = padded.shape
    row_count = row_total - 2
    outputs = weight.shape[0]
    wide = jnp.pad(padded, ((0, 0), (0, 0), (0, 0), (1, 1)))
    results = []
    for frame_pos in range(frame_count):
        total = jnp.zeros((outputs, row_count * col_count), jnp.float32)
        for row_shift in range(3):
            for col_shift in range(3):
                piece = wide[frame_pos, :, row_shift:row_shift + row_count, col_shift:col_shift + col_count]
                total = total + jnp.dot(weight[:, :, row_shift, col_shift], piece.reshape(channels, row_count * col_count), preferred_element_type=jnp.float32)
        results.append(total.reshape(outputs, row_count, col_count))
    return jnp.stack(results)

def grad_from_input(grad_out, padded):
    frame_count, channels, row_total, col_count = padded.shape
    row_count = row_total - 2
    outputs = grad_out.shape[1]
    wide = jnp.pad(padded, ((0, 0), (0, 0), (0, 0), (1, 1)))
    blocks = []
    for row_shift in range(3):
        for col_shift in range(3):
            total = jnp.zeros((outputs, channels), jnp.float32)
            for frame_pos in range(frame_count):
                piece = wide[frame_pos, :, row_shift:row_shift + row_count, col_shift:col_shift + col_count].reshape(channels, row_count * col_count)
                left = grad_out[frame_pos].reshape(outputs, row_count * col_count)
                total = total + lax.dot_general(left, piece, (((1,), (1,)), ((), ())), preferred_element_type=jnp.float32)
            blocks.append(total)
    return jnp.stack(blocks).reshape(3, 3, outputs, channels).transpose(2, 3, 0, 1)

def pool_mean(values):
    frame_count, channels, row_count, col_count = values.shape
    return values.reshape(frame_count, channels, row_count // 2, 2, col_count // 2, 2).mean(axis=(3, 5))

def upsample(values):
    return jnp.repeat(jnp.repeat(values, 2, 2), 2, 3)

def vgg_forward(image, weights):
    weight_one, bias_one, weight_two, bias_two, weight_three, bias_three, weight_four, bias_four = weights
    pre_one = conv_valid(pad_rows(image), weight_one) + bias_one[None, :, None, None]
    act_one = gelu_exact(pre_one).astype(jnp.bfloat16)
    pre_two = conv_valid(pad_rows(act_one), weight_two) + bias_two[None, :, None, None]
    act_two = gelu_exact(pre_two)
    pooled = pool_mean(act_two).astype(jnp.bfloat16)
    pre_three = conv_valid(pad_rows(pooled), weight_three) + bias_three[None, :, None, None]
    act_three = gelu_exact(pre_three).astype(jnp.bfloat16)
    pre_four = conv_valid(pad_rows(act_three), weight_four) + bias_four[None, :, None, None]
    act_four = gelu_exact(pre_four)
    return (pre_one, pre_two, act_two, pre_three, pre_four, act_four)

def lpips_layer(feat_dec, feat_tgt, lin, count):
    norm_dec = jnp.sqrt(lax.optimization_barrier(jnp.sum(feat_dec * feat_dec, 1, keepdims=True)) + 1e-06)
    norm_tgt = jnp.sqrt(lax.optimization_barrier(jnp.sum(feat_tgt * feat_tgt, 1, keepdims=True)) + 1e-06)
    unit_dec = feat_dec / norm_dec
    differ = unit_dec - feat_tgt / norm_tgt
    scaled = lin[None, :, None, None]
    part = jnp.sum(scaled * differ * differ) / count
    grad_unit = 2.0 * scaled * differ / count
    grad_feat = (grad_unit - unit_dec * lax.optimization_barrier(jnp.sum(grad_unit * unit_dec, 1, keepdims=True))) / norm_dec
    return (part, grad_feat)

def one_frame(pair, out_weight, out_bias, weights, lin_one, lin_two):
    features = pair[0][None]
    targets = pair[1][None]
    weight_one, bias_one, weight_two, bias_two, weight_three, bias_three, weight_four, bias_four = weights
    height = features.shape[2]
    width = features.shape[3]
    feat_pad = pad_rows(features)
    decoded = (conv_valid(feat_pad, out_weight) + out_bias[None, :, None, None]).astype(jnp.bfloat16)
    image_dec = ((decoded.astype(jnp.float32) - shift_array()) / scale_array()).astype(jnp.bfloat16)
    image_tgt = ((targets.astype(jnp.float32) - shift_array()) / scale_array()).astype(jnp.bfloat16)
    pre_one, pre_two, act_two, pre_three, pre_four, act_four = vgg_forward(image_dec, weights)
    tgt_acts = vgg_forward(image_tgt, weights)
    part_one, grad_two = lpips_layer(act_two, tgt_acts[2], lin_one, float(height * width))
    part_two, grad_four = lpips_layer(act_four, tgt_acts[5], lin_two, float(height // 2 * (width // 2)))
    grad_pre4 = (grad_four * gelu_slope(pre_four)).astype(jnp.bfloat16)
    grad_act3 = conv_valid(pad_rows(grad_pre4), flipped(weight_four))
    grad_pre3 = (grad_act3 * gelu_slope(pre_three)).astype(jnp.bfloat16)
    grad_pool = conv_valid(pad_rows(grad_pre3), flipped(weight_three))
    grad_pre2 = ((grad_two + 0.25 * upsample(grad_pool)) * gelu_slope(pre_two)).astype(jnp.bfloat16)
    grad_act1 = conv_valid(pad_rows(grad_pre2), flipped(weight_two))
    grad_pre1 = (grad_act1 * gelu_slope(pre_one)).astype(jnp.bfloat16)
    grad_image = conv_valid(pad_rows(grad_pre1), flipped(weight_one))
    grad_dec = (grad_image / scale_array()).astype(jnp.bfloat16)
    feature_grad = conv_valid(pad_rows(grad_dec), flipped(out_weight)).astype(jnp.bfloat16)
    weight_grad = grad_from_input(grad_dec, feat_pad)
    bias_grad = lax.optimization_barrier(jnp.sum(grad_dec.astype(jnp.float32), (0, 2, 3)))
    return (part_one + part_two, feature_grad[0], weight_grad, bias_grad)

def reference(features, out_weight, out_bias, targets, weight_one, bias_one, weight_two, bias_two, weight_three, bias_three, weight_four, bias_four, lin_one, lin_two):
    weights = (weight_one, bias_one, weight_two, bias_two, weight_three, bias_three, weight_four, bias_four)

    def runner(pair):
        return one_frame(pair, out_weight, out_bias, weights, lin_one, lin_two)
    parts, feature_grad, weight_grads, bias_grads = lax.map(runner, (features, targets))
    return (jnp.sum(parts), feature_grad, lax.optimization_barrier(jnp.sum(weight_grads, 0)), lax.optimization_barrier(jnp.sum(bias_grads, 0)))
```

```python
import functools
import math

import jax
import jax.numpy as jnp
from jax import lax
from jax.experimental import pallas as pl
from jax.experimental.pallas import tpu as pltpu
from jax.sharding import Mesh
from jax.sharding import PartitionSpec as P

CLIP = ("cx", "cz", "cc")
MESH = pl.DeviceIdType.MESH
F32 = jnp.float32
BF16 = jnp.bfloat16

shift_values = [-0.03, -0.088, -0.188]
scale_values = [0.458, 0.448, 0.45]

ROWS = 32
COLS = 96
HALO = 16
PROWS = ROWS // 2
PCOLS = COLS // 2
PHALO = HALO // 2
INV_SQRT2 = 1.0 / math.sqrt(2.0)
INV_SQRT2PI = 1.0 / math.sqrt(2.0 * math.pi)


def sub_vector(values):
    places = lax.broadcasted_iota(jnp.int32, (8, 1), 0)
    out = jnp.zeros((8, 1), F32)
    for i, value in enumerate(values):
        out = jnp.where(places == i, value, out)
    return out


def gelu_parts(v):
    phi = 0.5 + 0.5 * lax.erf(v * INV_SQRT2)
    return v * phi, phi


def slope_of(v, phi):
    return phi + v * (jnp.exp(v * v * -0.5) * INV_SQRT2PI)


def dot(a, b):
    return jnp.dot(a, b, preferred_element_type=F32)


def dot_tn(a, b):
    return lax.dot_general(a, b, (((0,), (0,)), ((), ())), preferred_element_type=F32)


def dot_nt(a, b):
    return lax.dot_general(a, b, (((1,), (1,)), ((), ())), preferred_element_type=F32)


def greet(barrier, axes):
    count = 0
    for axis in axes:
        n = lax.axis_size(axis)
        me = lax.axis_index(axis)
        for d in range(1, n):
            pl.semaphore_signal(
                barrier, inc=1, device_id={axis: lax.rem(me + d, n)}, device_id_type=MESH
            )
            count += 1
    return count


def decode_kernel(
    feat_ref, tgt_ref, wf_ref, bias_ref, xs_ref, win, rx, send_sem, recv_sem
):
    n = lax.axis_size("row")
    t = lax.axis_index("row")
    barrier = pltpu.get_barrier_semaphore()
    count = greet(barrier, ("row",))

    lane = lax.broadcasted_iota(jnp.int32, (8, 256), 1)
    wf = wf_ref[...]
    ys = [dot(wf, feat_ref[r]) for r in range(8)]
    tgt = tgt_ref[...].astype(F32)
    for rr in range(10):
        r = rr - 1
        parts = []
        for b in range(3):
            acc = None
            for a in range(3):
                src = r + a - 1
                if 0 <= src < 8:
                    k = (b * 3 + a) * 8
                    term = ys[src][k : k + 8]
                    acc = term if acc is None else acc + term
            parts.append(acc)
        left = jnp.where(lane == 0, 0.0, pltpu.roll(parts[0], 1, 1))
        right = jnp.where(lane == 255, 0.0, pltpu.roll(parts[2], 255, 1))
        out = parts[1] + left + right
        if 1 <= rr <= 8:
            out = out + jnp.concatenate(
                [jnp.zeros((3, 256), F32), tgt[:, r, :], jnp.zeros((2, 256), F32)], axis=0
            )
        for j in range(4):
            by = (32 - 64 * j) % 256
            moved = out if by == 0 else pltpu.roll(out, by, 1)
            win[j, rr] = moved[:, :128]

    pl.semaphore_wait(barrier, count)
    copies = []
    for d in range(1, n):
        j = lax.rem(t + d, n)
        copy = pltpu.make_async_remote_copy(
            src_ref=win.at[j],
            dst_ref=rx.at[t],
            send_sem=send_sem.at[d],
            recv_sem=recv_sem.at[d],
            device_id={"row": j},
            device_id_type=MESH,
        )
        copy.start()
        copies.append(copy)
    rx[t] = win[t]
    xs_ref[0] = jnp.zeros((24, 128), F32)
    xs_ref[ROWS + 1] = jnp.zeros((24, 128), F32)
    bias = sub_vector([bias_ref[0], bias_ref[1], bias_ref[2]])
    shift = sub_vector(shift_values + shift_values)
    places = lax.broadcasted_iota(jnp.int32, (8, 1), 0)
    scale = jnp.where(places >= 6, 1.0, sub_vector(scale_values + scale_values))
    col = lax.broadcasted_iota(jnp.int32, (8, 128), 1) + (64 * t - 32)
    inside = (col >= 0) & (col < 256)
    for copy in copies:
        copy.wait()
    for row in range(ROWS):
        s, k = divmod(row, 8)
        value = rx[s, k + 1]
        if k == 0 and s > 0:
            value = value + rx[s - 1, 9]
        if k == 7 and s < 3:
            value = value + rx[s + 1, 0]
        dec = (value + bias).astype(BF16).astype(F32)
        img = ((dec - shift) / scale).astype(BF16).astype(F32)
        img = jnp.where(inside, img, 0.0)
        xs_ref[row + 1] = jnp.concatenate(
            [pltpu.roll(img, 1, 1), img, pltpu.roll(img, 127, 1)], axis=0
        )


def store_shifted(buf, lead, row, value):
    size = value.shape[0]
    buf[lead + (0, row)] = pltpu.roll(value, 1, 0).astype(BF16)
    buf[lead + (1, row)] = value.astype(BF16)
    buf[lead + (2, row)] = pltpu.roll(value, size - 1, 0).astype(BF16)


def taps(buf, lead, row, rows):
    pieces = []
    for a in range(3):
        for b in range(3):
            piece = buf[lead + (b, pl.ds(row + a, rows))]
            pieces.append(piece.reshape(piece.shape[0] * piece.shape[1], piece.shape[2]))
    return jnp.concatenate(pieces, axis=1)


def vgg_kernel(
    count_one,
    count_two,
    xs_ref,
    w1_ref,
    w1b_ref,
    w2_ref,
    w3_ref,
    w4_ref,
    vec_ref,
    b3_ref,
    gd_ref,
    loss_ref,
    w2f,
    w2b,
    w3f,
    w3b,
    w4f,
    w4b,
    a1,
    sl1,
    sl2,
    gf1,
    p3,
    a3,
    sl3,
    g4,
    g3,
    g2,
    y1,
    fold,
):
    t = lax.axis_index("row")
    zero64 = jnp.zeros((64, 64), BF16)
    w2b[...] = jnp.zeros_like(w2b)
    w3f[...] = jnp.zeros_like(w3f)
    for a in range(3):
        for b in range(3):
            k = (a * 3 + b) * 128
            w = w2_ref[a, b]
            wt = w.astype(F32).T.astype(BF16)
            w2f[k : k + 64] = jnp.concatenate([wt, zero64], axis=1)
            w2f[k + 64 : k + 128] = jnp.concatenate([zero64, wt], axis=1)
            kb = a * 256 + b * 64
            w2b[kb : kb + 64] = jnp.concatenate([w2_ref[2 - a, 2 - b], zero64], axis=1)
            w3 = w3_ref[a, b]
            w3f[k : k + 64, 0:128] = w3
            w3f[k + 64 : k + 128, 128:256] = w3
            w3t = w3_ref[2 - a, 2 - b].astype(F32).T.astype(BF16)
            w3b[k : k + 128] = jnp.concatenate([w3t, jnp.zeros((128, 64), BF16)], axis=1)
            w4f[k : k + 128] = w4_ref[a, b].astype(F32).T.astype(BF16)
            w4b[k : k + 128] = w4_ref[2 - a, 2 - b]
    for buf in (p3, g4, g3):
        for b in range(3):
            for row in (0, PROWS + 1):
                buf[b, row] = jnp.zeros((PCOLS, 128), BF16)
    for m in range(2):
        for b in range(3):
            for row in (0, PROWS + 1):
                a3[m, b, row] = jnp.zeros((PCOLS, 128), BF16)
    for row in (0, ROWS + 1):
        for b in range(3):
            a1[b, row] = jnp.zeros((COLS, 128), BF16)
        g2[row] = jnp.zeros((COLS, 256), BF16)
        y1[row] = jnp.zeros((72, COLS), F32)
    loss_ref[...] = jnp.zeros_like(loss_ref)

    b1 = vec_ref[0:1]
    b2 = vec_ref[1:2]
    lin1 = vec_ref[2:3]
    lin2 = vec_ref[3:4]
    b4 = vec_ref[4:5]
    b3 = b3_ref[...]
    place = lax.broadcasted_iota(jnp.int32, (COLS, 1), 0)
    col = place + (64 * t - HALO)
    mask = ((col >= 0) & (col < 256)).astype(F32)
    own = ((place >= HALO) & (place < HALO + 64)).astype(F32)
    pplace = lax.broadcasted_iota(jnp.int32, (PCOLS, 1), 0)
    pcol = pplace + (32 * t - PHALO)
    pmask = ((pcol >= 0) & (pcol < 128)).astype(F32)
    pown = ((pplace >= PHALO) & (pplace < PHALO + 32)).astype(F32)
    row_half = lax.broadcasted_iota(jnp.int32, (128, 128), 0) < 64
    lane_half = lax.broadcasted_iota(jnp.int32, (128, 128), 1) < 64
    halves = jnp.where(row_half == lane_half, 1.0, 0.0).astype(BF16)
    ones = jnp.ones((128, 128), BF16)
    low = lax.broadcasted_iota(jnp.int32, (COLS, 128), 1) < 64

    def conv1(i, carry):
        for k in range(2):
            r = i * 2 + k
            x = jnp.concatenate([xs_ref[r], xs_ref[r + 1], xs_ref[r + 2]], axis=0)
            z = dot_tn(x.astype(BF16), w1_ref[...])[HALO : HALO + COLS] + b1
            act, phi = gelu_parts(z)
            sl1[r] = slope_of(z, phi)
            store_shifted(a1, (), r + 1, act * mask)
        return carry

    lax.fori_loop(0, ROWS // 2, conv1, 0)

    def conv2(i, carry):
        r = i * 4
        z = dot(taps(a1, (), r, 4), w2f[...]) + b2
        act, phi = gelu_parts(z)
        slope = slope_of(z, phi)
        inv = lax.rsqrt(dot((act * act).astype(BF16), halves) + 1e-06)
        unit = act * inv
        differ = unit - pltpu.roll(unit, 64, 1)
        scaled = lin1 * differ
        grad_unit = scaled * (2.0 / count_one)
        along = dot((grad_unit * unit).astype(BF16), halves)
        grad = (grad_unit - unit * along) * inv
        part = (scaled * differ).reshape(4, COLS, 128)
        part = part[0] + part[1] + part[2] + part[3]
        loss_ref[0:1] += jnp.sum(part * own, axis=0, keepdims=True) * (1.0 / count_one)
        sl2[pl.ds(r, 4)] = slope.reshape(4, COLS, 128)
        gf1[pl.ds(r, 4)] = grad.reshape(4, COLS, 128)
        act = act.reshape(4, COLS, 128)
        for k in range(2):
            fold[k] = act[2 * k] + act[2 * k + 1]
            pooled = (
                fold[k, pl.ds(0, PCOLS, 2)] + fold[k, pl.ds(1, PCOLS, 2)]
            ) * (0.25 * pmask)
            store_shifted(p3, (), i * 2 + k + 1, pooled)
        return carry

    lax.fori_loop(0, ROWS // 4, conv2, 0)

    def conv3(i, carry):
        r = i * 4
        z = dot(taps(p3, (), r, 4), w3f[...]) + b3
        act, phi = gelu_parts(z)
        dec = z[:, :128]
        sl3[pl.ds(r, 4)] = slope_of(dec, phi[:, :128]).reshape(4, PCOLS, 128)
        for m in range(2):
            one = act[:, m * 128 : m * 128 + 128].reshape(4, PCOLS, 128)
            for k in range(4):
                store_shifted(a3, (m,), r + k + 1, one[k] * pmask)
        return carry

    lax.fori_loop(0, PROWS // 4, conv3, 0)

    def conv4(i, carry):
        r = i * 4
        zd = dot(taps(a3, (0,), r, 4), w4f[...]) + b4
        zt = dot(taps(a3, (1,), r, 4), w4f[...]) + b4
        fd, phi = gelu_parts(zd)
        ft, _ = gelu_parts(zt)
        slope = slope_of(zd, phi)
        invd = lax.rsqrt(dot((fd * fd).astype(BF16), ones) + 1e-06)
        invt = lax.rsqrt(dot((ft * ft).astype(BF16), ones) + 1e-06)
        unit = fd * invd
        differ = unit - ft * invt
        scaled = lin2 * differ
        grad_unit = scaled * (2.0 / count_two)
        along = dot((grad_unit * unit).astype(BF16), ones)
        grad = (grad_unit - unit * along) * invd * slope
        part = (scaled * differ).reshape(4, PCOLS, 128)
        part = part[0] + part[1] + part[2] + part[3]
        loss_ref[1:2] += jnp.sum(part * pown, axis=0, keepdims=True) * (1.0 / count_two)
        grad = grad.reshape(4, PCOLS, 128)
        for k in range(4):
            store_shifted(g4, (), r + k + 1, grad[k] * pmask)
        return carry

    lax.fori_loop(0, PROWS // 4, conv4, 0)

    def back4(i, carry):
        r = i * 4
        z = dot(taps(g4, (), r, 4), w4b[...]).reshape(4, PCOLS, 128)
        for k in range(4):
            store_shifted(g3, (), r + k + 1, z[k] * sl3[r + k] * pmask)
        return carry

    lax.fori_loop(0, PROWS // 4, back4, 0)

    def back3(i, carry):
        r = i * 4
        z = (dot(taps(g3, (), r, 4), w3b[...]) * 0.25).reshape(4, PCOLS, 128)
        for k in range(4):
            fold[k, pl.ds(0, PCOLS, 2)] = z[k]
            fold[k, pl.ds(1, PCOLS, 2)] = z[k]
            up = fold[k]
            for h in range(2):
                row = (r + k) * 2 + h
                g = (gf1[row] + up) * sl2[row] * mask
                before = pltpu.roll(g, 1, 0)
                after = pltpu.roll(g, COLS - 1, 0)
                g2[row + 1, :, 0:128] = jnp.where(low, before, pltpu.roll(g, 64, 1)).astype(BF16)
                g2[row + 1, :, 128:256] = jnp.where(low, after, 0.0).astype(BF16)
        return carry

    lax.fori_loop(0, PROWS // 4, back3, 0)

    def back2(i, carry):
        r = i * 4
        pieces = [g2[pl.ds(r + a, 4)].reshape(4 * COLS, 256) for a in range(3)]
        z = dot(jnp.concatenate(pieces, axis=1), w2b[...]).reshape(4, COLS, 128)
        for k in range(4):
            g1 = (z[k] * sl1[r + k] * mask).astype(BF16)
            y1[r + k + 1] = dot_nt(w1b_ref[...], g1)
        return carry

    lax.fori_loop(0, ROWS // 4, back2, 0)

    places = lax.broadcasted_iota(jnp.int32, (8, 1), 0)
    scale = jnp.where(places >= 3, 1.0, sub_vector(scale_values))
    half = lax.rem(t, 2)
    lane = lax.broadcasted_iota(jnp.int32, (8, 128), 1)
    mine = (lane >= 64 * half) & (lane < 64 * half + 64)
    gd_ref[0] = jnp.zeros((8, 128), F32)
    gd_ref[ROWS + 1] = jnp.zeros((8, 128), F32)
    pad = jnp.zeros((8, 128 - COLS), F32)

    def finish(r, carry):
        parts = []
        for b in range(3):
            acc = None
            for a in range(3):
                k = (b * 3 + a) * 8
                term = y1[r + a, k : k + 8]
                acc = term if acc is None else acc + term
            parts.append(jnp.concatenate([acc, pad], axis=1))
        out = parts[1] + pltpu.roll(parts[0], 1, 1) + pltpu.roll(parts[2], 127, 1)
        out = (out / scale).astype(BF16).astype(F32)
        out = pltpu.roll(out, lax.rem(64 * half + 128 - HALO, 128), 1)
        gd_ref[r + 1] = jnp.where(mine, out, 0.0)
        return carry

    lax.fori_loop(0, ROWS, finish, 0)


AXES = ("cc", "row", "cx", "cz")


def finish_kernel(
    sizes,
    gd_ref,
    feat_ref,
    wf_ref,
    loss_ref,
    fg_ref,
    sum_ref,
    rx,
    acc,
    gs,
    send_sem,
    recv_sem,
    *rest,
):
    bufs = rest[: len(AXES)]
    sems = rest[len(AXES) :]
    n = lax.axis_size("row")
    t = lax.axis_index("row")
    barrier = pltpu.get_barrier_semaphore()
    count = greet(barrier, AXES)
    pl.semaphore_wait(barrier, count)
    copies = []
    for d in range(1, n):
        j = lax.rem(t + d, n)
        copy = pltpu.make_async_remote_copy(
            src_ref=gd_ref.at[pl.ds(8 * j, 10)],
            dst_ref=rx.at[t],
            send_sem=send_sem.at[d],
            recv_sem=recv_sem.at[d],
            device_id={"row": j},
            device_id_type=MESH,
        )
        copy.start()
        copies.append(copy)
    rx[t] = gd_ref[pl.ds(8 * t, 10)]
    for copy in copies:
        copy.wait()

    lane = lax.broadcasted_iota(jnp.int32, (8, 256), 1)
    shifted = []
    for rr in range(10):
        g = jnp.concatenate([rx[0, rr] + rx[1, rr], rx[2, rr] + rx[3, rr]], axis=1)
        after = jnp.where(lane == 255, 0.0, pltpu.roll(g, 255, 1))
        before = jnp.where(lane == 0, 0.0, pltpu.roll(g, 1, 1))
        shifted.append((after, g, before))
    grad = jnp.zeros((72, 128), F32)
    for r in range(8):
        g = jnp.concatenate(
            [shifted[r - a + 2][b] for b in range(3) for a in range(3)], axis=0
        ).astype(BF16)
        gs[r] = g
        grad = grad + dot_nt(g, feat_ref[r])
    own = shifted[1][1]
    for rr in range(2, 9):
        own = own + shifted[rr][1]
    bias = jnp.sum(own, axis=1, keepdims=True)
    lane8 = lax.broadcasted_iota(jnp.int32, (8, 128), 1)
    sub8 = lax.broadcasted_iota(jnp.int32, (8, 128), 0)
    spread = jnp.where((lane8 == sub8) & (sub8 < 3), bias, 0.0)
    part = jnp.sum(loss_ref[...])
    spread = jnp.where((sub8 == 3) & (lane8 == 3), part, spread)
    acc[24:32] = jnp.zeros((8, 128), F32)
    for k in range(9):
        acc[3 * k : 3 * k + 3] = grad[8 * k : 8 * k + 3]
    acc[27:28] = jnp.sum(spread, axis=0, keepdims=True)

    first = True
    for i, axis in enumerate(AXES):
        size = sizes[i]
        me = lax.axis_index(axis)
        buf = bufs[i]
        if size > 1:
            buf[me] = acc[...]
            copies = []
            for d in range(1, size):
                j = lax.rem(me + d, size)
                copy = pltpu.make_async_remote_copy(
                    src_ref=buf.at[me],
                    dst_ref=buf.at[me],
                    send_sem=sems[2 * i].at[d],
                    recv_sem=sems[2 * i + 1].at[d],
                    device_id={axis: j},
                    device_id_type=MESH,
                )
                copy.start()
                copies.append(copy)
        if first:
            first = False
            for r in range(8):
                fg_ref[r] = dot_tn(wf_ref[...], gs[r]).astype(BF16)
        if size > 1:
            for copy in copies:
                copy.wait()
            total = buf[0]
            for k in range(1, size):
                total = total + buf[k]
            acc[...] = total
    sum_ref[...] = acc[...]


def vmem(count):
    return [pl.BlockSpec(memory_space=pltpu.VMEM)] * count


def local(
    features,
    out_weight,
    out_bias,
    targets,
    weight_one,
    bias_one,
    weight_two,
    bias_two,
    weight_three,
    bias_three,
    weight_four,
    bias_four,
    lin_one,
    lin_two,
):
    height = features.shape[2] * lax.axis_size("row")
    width = features.shape[3]
    count_one = float(height * width)
    count_two = float((height // 2) * (width // 2))
    feat = features[0].transpose(1, 0, 2)
    wf = jnp.pad(out_weight.transpose(3, 2, 0, 1), ((0, 0), (0, 0), (0, 5), (0, 0)))
    wf = wf.reshape(72, 128)
    w1 = weight_one.transpose(2, 3, 1, 0)
    w1 = jnp.concatenate(
        [
            jnp.pad(w1, ((0, 0), (0, 0), (0, 0), (0, 64))),
            jnp.pad(w1, ((0, 0), (0, 0), (0, 2), (64, 0))),
        ],
        axis=2,
    ).reshape(72, 128)
    w1b = jnp.flip(weight_one, (2, 3)).transpose(3, 2, 1, 0)
    w1b = jnp.pad(w1b, ((0, 0), (0, 0), (0, 5), (0, 64))).reshape(72, 128)
    zero = jnp.zeros((64,), F32)
    vec = jnp.stack(
        [
            jnp.concatenate([bias_one, bias_one]),
            jnp.concatenate([bias_two, bias_two]),
            jnp.concatenate([lin_one, zero]),
            lin_two,
            bias_four,
        ]
    )
    b3 = jnp.concatenate([bias_three, bias_three])[None]

    xs = pl.pallas_call(
        decode_kernel,
        out_shape=jax.ShapeDtypeStruct((ROWS + 2, 24, 128), F32),
        in_specs=vmem(3) + [pl.BlockSpec(memory_space=pltpu.SMEM)],
        out_specs=vmem(1)[0],
        scratch_shapes=[
            pltpu.VMEM((4, 10, 8, 128), F32),
            pltpu.VMEM((4, 10, 8, 128), F32),
            pltpu.SemaphoreType.DMA((4,)),
            pltpu.SemaphoreType.DMA((4,)),
        ],
        compiler_params=pltpu.CompilerParams(collective_id=0, has_side_effects=True),
        name="decode",
    )(feat, targets[0], wf, out_bias)

    gd, loss = pl.pallas_call(
        functools.partial(vgg_kernel, count_one, count_two),
        out_shape=(
            jax.ShapeDtypeStruct((ROWS + 2, 8, 128), F32),
            jax.ShapeDtypeStruct((8, 128), F32),
        ),
        in_specs=vmem(8),
        out_specs=tuple(vmem(2)),
        scratch_shapes=[
            pltpu.VMEM((1152, 128), BF16),
            pltpu.VMEM((768, 128), BF16),
            pltpu.VMEM((1152, 256), BF16),
            pltpu.VMEM((1152, 128), BF16),
            pltpu.VMEM((1152, 128), BF16),
            pltpu.VMEM((1152, 128), BF16),
            pltpu.VMEM((3, ROWS + 2, COLS, 128), BF16),
            pltpu.VMEM((ROWS, COLS, 128), F32),
            pltpu.VMEM((ROWS, COLS, 128), F32),
            pltpu.VMEM((ROWS, COLS, 128), F32),
            pltpu.VMEM((3, PROWS + 2, PCOLS, 128), BF16),
            pltpu.VMEM((2, 3, PROWS + 2, PCOLS, 128), BF16),
            pltpu.VMEM((PROWS, PCOLS, 128), F32),
            pltpu.VMEM((3, PROWS + 2, PCOLS, 128), BF16),
            pltpu.VMEM((3, PROWS + 2, PCOLS, 128), BF16),
            pltpu.VMEM((ROWS + 2, COLS, 256), BF16),
            pltpu.VMEM((ROWS + 2, 72, COLS), F32),
            pltpu.VMEM((4, COLS, 128), F32),
        ],
        name="vgg",
    )(
        xs,
        w1,
        w1b,
        weight_two.transpose(2, 3, 0, 1),
        weight_three.transpose(2, 3, 1, 0),
        weight_four.transpose(2, 3, 0, 1),
        vec,
        b3,
    )

    sizes = tuple(lax.axis_size(axis) for axis in AXES)
    fg, total = pl.pallas_call(
        functools.partial(finish_kernel, sizes),
        out_shape=(
            jax.ShapeDtypeStruct((8, 128, 256), BF16),
            jax.ShapeDtypeStruct((32, 128), F32),
        ),
        in_specs=vmem(4),
        out_specs=tuple(vmem(2)),
        scratch_shapes=[
            pltpu.VMEM((4, 10, 8, 128), F32),
            pltpu.VMEM((32, 128), F32),
            pltpu.VMEM((8, 72, 256), BF16),
            pltpu.SemaphoreType.DMA((4,)),
            pltpu.SemaphoreType.DMA((4,)),
        ]
        + [pltpu.VMEM((size, 32, 128), F32) for size in sizes]
        + [pltpu.SemaphoreType.DMA((size,)) for size in sizes for _ in range(2)],
        compiler_params=pltpu.CompilerParams(collective_id=1, has_side_effects=True),
        name="finish",
    )(gd, feat, wf, loss)

    weight_total = total[:27].reshape(3, 3, 3, 128).transpose(2, 3, 1, 0)
    return (total[27, 3], fg.transpose(1, 0, 2)[None], weight_total, total[27, 0:3])


def build(torus):
    placed = [P()] * 14
    placed[0] = P(CLIP, None, "row", None)
    placed[3] = P(CLIP, None, "row", None)
    return jax.shard_map(
        local,
        mesh=torus,
        in_specs=tuple(placed),
        out_specs=(P(), P(CLIP, None, "row", None), P(), P()),
        check_vma=False,
    )


def solution(mesh):
    torus = Mesh(mesh.devices.reshape(4, 8, 2, mesh.shape["row"]), CLIP + ("row",))
    return build(torus)
```
